256 devices in a mesh: dp: 8 (over z_lo, core), ctx: 32 (over x, y, z_hi).
Axes of the slice: x: 4, y: 4, z: 8 (z_hi: 2, z_lo: 4; z = z_hi * 4 + z_lo), core: 2. Of those that a mesh axis runs over, the one named last changes fastest.
Arguments:
- doc_lengths: int32 [64], P('dp'), parts along dimension 0, may hold values from 1 to 1024, 4096 in all
- assignment: int32 [1024], P('dp'), parts along dimension 0, may hold values from 0 to 127, each once
- queries: bfloat16 [32768, 4096], P(('dp', 'ctx')), parts along dimension 0, may hold values from -6 to 6
- key_state_rows: bfloat16 [32768, 512], P(('dp', 'ctx')), parts along dimension 0, may hold values from -6 to 6
- value_state_rows: bfloat16 [32768, 512], P(('dp', 'ctx')), parts along dimension 0, may hold values from -6 to 6
- out_grad: bfloat16 [32768, 4096], P(('dp', 'ctx')), parts along dimension 0, may hold values from -6 to 6
Outputs:
- attention_out: bfloat16 [32768, 4096], P(('dp', 'ctx')), parts along dimension 0
- query_grad: bfloat16 [32768, 4096], P(('dp', 'ctx')), parts along dimension 0
- key_gradient: bfloat16 [32768, 512], P(('dp', 'ctx')), parts along dimension 0
- value_gradient: bfloat16 [32768, 512], P(('dp', 'ctx')), parts along dimension 0
The draws below stay inside these ranges and needn't reach their ends.
There are 8 independent parts, one for each index of `dp`. The reference program is written for one: setup_inputs(seed, part) draws one part's arguments, and reference() takes and returns one part's arrays. A program takes and returns all parts, laid end to end along the dimension named above; each array names one. Nothing has to cross between parts.
Inputs may be any that keep to these rules, and one draw needn't show every extreme that they name: `assignment`: each of 0 to 127 once.
All inputs are finite; a program needn't handle non-finite values.
Results may differ from the reference program's by a relative error of at most 0.015.
Values may be sent and summed in bfloat16 or wider, within the bound.
No kernel may reach another device: no remote copies, remote signals or barrier semaphores. Data moves between devices by JAX's collectives and lax.ppermute only.
A program may use at most 128 MiB of HBM per device.

```python
import math
import jax
import jax.numpy as jnp
import numpy as np
from jax import lax

DEVICE_TOKENS = 128
BLK = 32
MOST = 1024
QUERY_HEADS = 32
KEY_VALUE_HEADS = 4
HEAD_SIZE = 128
PACK_TOKENS = 4096
NBLK = 128
NDOC = 8
N_CTX = 32


def drawn_pair(key):
    base = jax.random.fold_in(key, 7)
    key_listing = jax.random.split(base, 4)
    query_draw = jnp.clip(jax.random.normal(key_listing[2], (PACK_TOKENS, QUERY_HEADS * HEAD_SIZE), jnp.float32), -6.0, 6.0)
    key_sample = jnp.clip(jax.random.normal(key_listing[3], (PACK_TOKENS, KEY_VALUE_HEADS * HEAD_SIZE), jnp.float32), -6.0, 6.0)
    return (query_draw, key_sample)


def draw_queries(key, part):
    return drawn_pair(key)[0].astype(jnp.bfloat16)


def draw_key_state_rows(key, part):
    return drawn_pair(key)[1].astype(jnp.bfloat16)


def steps_of(own_key, extent, shards, smallest, largest):
    level, own = 1.0, jax.random.fold_in(own_key, 6)
    for position, shards_of in shards:
        draws = jnp.exp(jax.random.uniform(jax.random.fold_in(own, position), (shards_of,), jnp.float32, smallest / len(shards), largest / len(shards)))
        level = level * jnp.repeat(draws, extent[position] // shards_of).reshape([-1 if axis == position else 1 for axis in range(len(extent))])
    return level


def split_up(amount, total, bound, lean):
    weights = [(1 << 20) // math.isqrt(standing ** lean) + 1 for standing in range(2, amount + 1)]
    surplus, given = total - bound - (amount - 1), [1] * (amount - 1)
    while surplus > 0:
        movable = [i for i in range(amount - 1) if given[i] < bound]
        whole, budget = sum([weights[i] for i in movable]), surplus
        for i in movable:
            more = min(bound - given[i], max(1, budget * weights[i] // whole), surplus)
            given[i] = given[i] + more
            surplus = surplus - more
    return np.array([bound] + given)


def uneven(rng, number_of, total, bound, lean):
    if number_of == 2:
        one = jax.random.randint(rng, (), max(1, total - bound), min(bound, total - 1) + 1)
        return jnp.stack([one, total - one])
    lengths = jnp.asarray(split_up(number_of, total, bound, lean), jnp.int32)
    couples = (number_of - 1) // 2
    source_of, receiver = lengths[1:1 + 2 * couples:2], lengths[2:2 + 2 * couples:2]
    margin = jnp.minimum(source_of - 1, bound - receiver)
    shifted = jax.random.randint(jax.random.fold_in(rng, 1), (couples,), 0, 1 << 20) % (margin + 1)
    lengths = lengths.at[1:1 + 2 * couples:2].set(source_of - shifted).at[2:2 + 2 * couples:2].set(receiver + shifted)
    return lengths[jax.random.permutation(jax.random.fold_in(rng, 2), number_of)]


def noise(stream_key, shape, scale, most, pieces=(), kind=jnp.bfloat16):
    entries = scale * jax.random.normal(stream_key, shape, jnp.float32)
    if pieces:
        entries = entries * steps_of(stream_key, shape, pieces, -0.22, 0.18)
    return jnp.clip(entries, -most, most).astype(kind)


def setup_inputs(seed: int = 0, part: int = 0) -> dict:
    seeds = jax.random.split(jax.random.key(seed), 7)
    own_keys = jax.random.split(jax.random.fold_in(seeds[6], part), 7)
    doc_lengths = uneven(own_keys[0], NDOC, PACK_TOKENS, MOST, 2).astype(jnp.int32)
    assignment = jax.random.permutation(own_keys[1], NBLK).astype(jnp.int32)
    queries = draw_queries(jax.random.fold_in(jax.random.fold_in(seeds[6], part), 71), part)
    key_state_rows = draw_key_state_rows(jax.random.fold_in(jax.random.fold_in(seeds[6], part), 71), part)
    value_state_rows = noise(own_keys[4], (PACK_TOKENS, KEY_VALUE_HEADS * HEAD_SIZE), 1.0, 6.0, ((0, 32),))
    out_grad = noise(own_keys[5], (PACK_TOKENS, QUERY_HEADS * HEAD_SIZE), 1.0, 6.0, ((0, 32),))
    return dict(doc_lengths=doc_lengths, assignment=assignment, queries=queries, key_state_rows=key_state_rows, value_state_rows=value_state_rows, out_grad=out_grad)


def rounded(values):
    return lax.optimization_barrier(values.astype(jnp.bfloat16)).astype(jnp.float32)


def places_of(assignment):
    slot_rows = jnp.arange(PACK_TOKENS, dtype=jnp.int32)
    return (assignment[slot_rows // BLK] * BLK + slot_rows % BLK).astype(jnp.int32)


def documents_of(doc_lengths, places):
    doc_bounds = jnp.cumsum(doc_lengths).astype(jnp.int32)
    return jnp.sum((doc_bounds[None, :] <= places[:, None]).astype(jnp.int32), axis=1)


def reference(doc_lengths, assignment, queries, key_state_rows, value_state_rows, out_grad):
    group_width = QUERY_HEADS // KEY_VALUE_HEADS
    score_scale = HEAD_SIZE ** -0.5
    key_places = places_of(assignment)
    doc_ids = documents_of(doc_lengths, key_places)
    key_complete = key_state_rows.reshape(PACK_TOKENS, KEY_VALUE_HEADS, HEAD_SIZE).astype(jnp.float32)
    value_complete = value_state_rows.reshape(PACK_TOKENS, KEY_VALUE_HEADS, HEAD_SIZE).astype(jnp.float32)

    def device_step(grand_totals, slices):
        query_piece, gradient_piece, query_place, query_doc = slices
        query_float = query_piece.reshape(DEVICE_TOKENS, KEY_VALUE_HEADS, group_width, HEAD_SIZE).astype(jnp.float32)
        gradient_float = gradient_piece.reshape(DEVICE_TOKENS, KEY_VALUE_HEADS, group_width, HEAD_SIZE).astype(jnp.float32)
        scores = jnp.einsum('qgjd,kgd->gjqk', query_float, key_complete) * score_scale
        allowed = (doc_ids[None, :] == query_doc[:, None]) & (key_places[None, :] <= query_place[:, None])
        masked = jnp.where(allowed, scores, -jnp.inf)
        row_top = jnp.max(masked, axis=-1, keepdims=True)
        log_total = row_top + jnp.log(jnp.sum(jnp.exp(masked - row_top), axis=-1, keepdims=True))
        attention = jnp.where(allowed, jnp.exp(scores - log_total), 0.0)
        attention_b = rounded(attention)
        output = jnp.einsum('gjqk,kgd->qgjd', attention_b, value_complete).astype(jnp.bfloat16)
        row_delta = jnp.sum(gradient_float * output.astype(jnp.float32), axis=-1)
        row_delta = jnp.transpose(row_delta, (1, 2, 0))[..., None]
        grad_weights = jnp.einsum('qgjd,kgd->gjqk', gradient_float, value_complete)
        dscore = rounded(attention * (grad_weights - row_delta) * score_scale)
        query_term = jnp.einsum('gjqk,kgd->qgjd', dscore, key_complete).astype(jnp.bfloat16)
        key_term = rounded(jnp.einsum('gjqk,qgjd->kgd', dscore, query_float))
        value_term = rounded(jnp.einsum('gjqk,qgjd->kgd', attention_b, gradient_float))
        grand_totals = (grand_totals[0] + key_term, grand_totals[1] + value_term)
        return grand_totals, (output.reshape(DEVICE_TOKENS, QUERY_HEADS * HEAD_SIZE), query_term.reshape(DEVICE_TOKENS, QUERY_HEADS * HEAD_SIZE))

    slices = (queries.reshape(N_CTX, DEVICE_TOKENS, QUERY_HEADS * HEAD_SIZE), out_grad.reshape(N_CTX, DEVICE_TOKENS, QUERY_HEADS * HEAD_SIZE),
              key_places.reshape(N_CTX, DEVICE_TOKENS), doc_ids.reshape(N_CTX, DEVICE_TOKENS))
    initial_sums = (jnp.zeros((PACK_TOKENS, KEY_VALUE_HEADS, HEAD_SIZE), jnp.float32), jnp.zeros((PACK_TOKENS, KEY_VALUE_HEADS, HEAD_SIZE), jnp.float32))
    grand_totals, stacked = lax.scan(device_step, initial_sums, slices)
    attention_out = stacked[0].reshape(PACK_TOKENS, QUERY_HEADS * HEAD_SIZE)
    query_grad = stacked[1].reshape(PACK_TOKENS, QUERY_HEADS * HEAD_SIZE)
    key_gradient = grand_totals[0].reshape(PACK_TOKENS, KEY_VALUE_HEADS * HEAD_SIZE).astype(jnp.bfloat16)
    value_gradient = grand_totals[1].reshape(PACK_TOKENS, KEY_VALUE_HEADS * HEAD_SIZE).astype(jnp.bfloat16)
    return attention_out, query_grad, key_gradient, value_gradient
```

```python
import functools

import jax
import jax.numpy as jnp
from jax import lax
from jax.experimental import pallas as pl
from jax.experimental.pallas import tpu as pltpu
from jax.sharding import Mesh
from jax.sharding import PartitionSpec as P

BLK = 32
HEAD = 128
TILE = 256


def attend(assign_ref, len_ref, coord_ref, qd_ref, kv_ref, od_ref, dkv_ref,
           kp, vp, kt, vt, dk, dv, s_scr, dp_scr, ot, dqt, *, docs, slots, group, xs, ys, zs):
    scale = HEAD ** -0.5
    i = pl.program_id(0)
    per = slots // (xs * ys * zs)
    z = coord_ref[1]
    rows = group * BLK
    tile_blocks = TILE // BLK

    def place(s):
        c = s // per
        zz = jnp.where(c % zs == z, 0, 1)
        return (((c // zs) % ys) * zs + zz) * (xs * per) + (c // (ys * zs)) * per + s % per

    @pl.when(i == 0)
    def _():
        def bring(s, carry):
            b = assign_ref[s]
            at = place(s)
            kp[b] = kv_ref[at, :, :HEAD]
            vp[b] = kv_ref[at, :, HEAD:]
            dk[b] = jnp.zeros((BLK, HEAD), jnp.float32)
            dv[b] = jnp.zeros((BLK, HEAD), jnp.float32)
            return carry
        lax.fori_loop(0, slots, bring, 0, unroll=8)

        def flip(t, carry):
            kt[t] = kp[pl.ds(t * tile_blocks, tile_blocks)].reshape(TILE, HEAD).T
            vt[t] = vp[pl.ds(t * tile_blocks, tile_blocks)].reshape(TILE, HEAD).T
            return carry
        lax.fori_loop(0, slots * BLK // TILE, flip, 0)

    slot = ((i // per) * (ys * zs) + coord_ref[0]) * per + i % per
    first = assign_ref[slot] * BLK
    place_row = first + (lax.broadcasted_iota(jnp.int32, (1, rows), 1) % BLK)
    start_row = jnp.zeros((1, rows), jnp.int32)
    start = jnp.int32(0)
    bound = jnp.int32(0)
    for d in range(docs):
        bound = bound + len_ref[d]
        start_row = jnp.where(place_row >= bound, bound, start_row)
        start = jnp.where(first >= bound, bound, start)
    t0 = start // TILE
    t1 = (first + BLK - 1) // TILE + 1

    q = jnp.concatenate([qd_ref[0, :, h * HEAD:(h + 1) * HEAD] for h in range(group)], axis=0)
    do = jnp.concatenate([qd_ref[0, :, (group + h) * HEAD:(group + h + 1) * HEAD] for h in range(group)], axis=0)
    NT = (((1,), (1,)), ((), ()))
    NN = (((1,), (0,)), ((), ()))
    dot = functools.partial(lax.dot_general, preferred_element_type=jnp.float32)

    def score(t, top):
        k_t = kp[pl.ds(t * tile_blocks, tile_blocks)].reshape(TILE, HEAD)
        v_t = vp[pl.ds(t * tile_blocks, tile_blocks)].reshape(TILE, HEAD)
        s = dot(k_t, q, NT)
        key = t * TILE + lax.broadcasted_iota(jnp.int32, (TILE, rows), 0)
        s = jnp.where((key >= start_row) & (key <= place_row), s, -jnp.inf)
        s_scr[t - t0] = s
        dp_scr[t - t0] = dot(v_t, do, NT)
        return jnp.maximum(top, jnp.max(s.reshape(TILE // 8, 8, rows), axis=0))

    top = lax.fori_loop(t0, t1, score, jnp.full((8, rows), -jnp.inf, jnp.float32))
    top = jnp.max(top, axis=0, keepdims=True)

    def total(t, sums):
        e = jnp.exp((s_scr[t - t0] - top) * scale)
        s_scr[t - t0] = e
        ed = e * dp_scr[t - t0]
        return (sums[0] + jnp.sum(e.reshape(TILE // 8, 8, rows), axis=0),
                sums[1] + jnp.sum(ed.reshape(TILE // 8, 8, rows), axis=0))

    zero = jnp.zeros((8, rows), jnp.float32)
    sums = lax.fori_loop(t0, t1, total, (zero, zero))
    inv = 1.0 / jnp.sum(sums[0], axis=0, keepdims=True)
    delta = jnp.sum(sums[1], axis=0, keepdims=True) * inv
    ot[...] = jnp.zeros_like(ot)
    dqt[...] = jnp.zeros_like(dqt)

    def grads(t, carry):
        p = s_scr[t - t0] * inv
        pb = p.astype(jnp.bfloat16)
        ds = (p * (dp_scr[t - t0] - delta) * scale).astype(jnp.bfloat16)
        ot[...] += dot(vt[t], pb, NN)
        dqt[...] += dot(kt[t], ds, NN)
        at = pl.ds(t * tile_blocks, tile_blocks)
        dv[at] += dot(pb, do, NN).reshape(tile_blocks, BLK, HEAD)
        dk[at] += dot(ds, q, NN).reshape(tile_blocks, BLK, HEAD)
        return carry

    lax.fori_loop(t0, t1, grads, 0)
    o = ot[...].T.astype(jnp.bfloat16)
    dq = dqt[...].T.astype(jnp.bfloat16)
    for h in range(group):
        od_ref[0, :, h * HEAD:(h + 1) * HEAD] = o[h * BLK:(h + 1) * BLK]
        od_ref[0, :, (group + h) * HEAD:(group + h + 1) * HEAD] = dq[h * BLK:(h + 1) * BLK]

    @pl.when(i == pl.num_programs(0) - 1)
    def _():
        def send(s, carry):
            b = assign_ref[s]
            at = place(s)
            dkv_ref[at, :, :HEAD] = dk[b].astype(jnp.bfloat16)
            dkv_ref[at, :, HEAD:] = dv[b].astype(jnp.bfloat16)
            return carry
        lax.fori_loop(0, slots, send, 0, unroll=8)


def attention(assign, lengths, coord, qd, kv, *, xs, ys, zs):
    blocks = qd.shape[0]
    group = qd.shape[2] // (2 * HEAD)
    slots = kv.shape[0]
    span = (1023 + BLK + TILE - 1) // TILE + 1
    rows = group * BLK
    f32, bf = jnp.float32, jnp.bfloat16
    body = functools.partial(attend, docs=lengths.shape[0], slots=slots, group=group, xs=xs, ys=ys, zs=zs)
    return pl.pallas_call(
        body,
        out_shape=(jax.ShapeDtypeStruct(qd.shape, bf), jax.ShapeDtypeStruct(kv.shape, bf)),
        grid_spec=pltpu.PrefetchScalarGridSpec(
            num_scalar_prefetch=3, grid=(blocks,),
            in_specs=[pl.BlockSpec((1, BLK, qd.shape[2]), lambda i, *_: (i, 0, 0)),
                      pl.BlockSpec(kv.shape, lambda i, *_: (0, 0, 0))],
            out_specs=[pl.BlockSpec((1, BLK, qd.shape[2]), lambda i, *_: (i, 0, 0)),
                       pl.BlockSpec(kv.shape, lambda i, *_: (0, 0, 0))],
            scratch_shapes=[
                pltpu.VMEM((slots, BLK, HEAD), bf), pltpu.VMEM((slots, BLK, HEAD), bf),
                pltpu.VMEM((slots * BLK // TILE, HEAD, TILE), bf), pltpu.VMEM((slots * BLK // TILE, HEAD, TILE), bf),
                pltpu.VMEM((slots, BLK, HEAD), f32), pltpu.VMEM((slots, BLK, HEAD), f32),
                pltpu.VMEM((span, TILE, rows), f32), pltpu.VMEM((span, TILE, rows), f32),
                pltpu.VMEM((HEAD, rows), f32), pltpu.VMEM((HEAD, rows), f32),
            ]),
        compiler_params=pltpu.CompilerParams(dimension_semantics=("arbitrary",), vmem_limit_bytes=48 << 20),
        name="attend",
    )(assign, lengths, coord, qd, kv)


X, Y, Z = "ctx_0", "ctx_1", "ctx_2"
DP_CTX = ("dp", X, Y, Z)
SWAP = [(0, 1), (1, 0)]


def by_head(a, heads):
    return a.reshape(a.shape[0], heads, a.shape[1] // heads).transpose(1, 0, 2)


def by_row(a):
    return a.transpose(1, 0, 2).reshape(a.shape[1], a.shape[0] * a.shape[2])


def body(doc_lengths, assignment, queries, key_state_rows, value_state_rows, out_grad):
    xs, ys, zs = (lax.axis_size(name) for name in (X, Y, Z))
    rows = queries.shape[0]
    slots = assignment.shape[0]
    coord = jnp.stack([lax.axis_index((Y, Z)), lax.axis_index(Z)]).astype(jnp.int32)

    kv = jnp.concatenate([by_head(key_state_rows, xs), by_head(value_state_rows, xs)], axis=2)
    qd = jnp.concatenate([by_head(queries, xs), by_head(out_grad, xs)], axis=2)
    kv = lax.all_to_all(kv, X, 0, 0, tiled=True)
    qd, kv = lax.optimization_barrier((qd, kv))
    peer = lax.ppermute(kv, Z, SWAP)
    qd = lax.all_to_all(qd, X, 0, 0, tiled=True)
    pair = jnp.stack([kv, peer])
    pair, qd = lax.optimization_barrier((pair, qd))
    pairs = jnp.broadcast_to(pair[None], (ys,) + pair.shape)
    pairs = lax.all_to_all(pairs, Y, 0, 0, tiled=True)

    od, dkv = attention(
        assignment,
        doc_lengths,
        coord,
        qd.reshape(xs * rows // BLK, BLK, -1),
        pairs.reshape(slots, BLK, -1),
        xs=xs,
        ys=ys,
        zs=zs,
    )

    dkv = dkv.reshape(pairs.shape)
    dkv = lax.all_to_all(dkv, Y, 0, 0, tiled=True)
    dkv = jnp.sum(dkv.astype(jnp.float32), axis=0)
    other = dkv[1].astype(jnp.bfloat16)
    other, od = lax.optimization_barrier((other, od))
    other = lax.ppermute(other, Z, SWAP)
    od = lax.all_to_all(od.reshape(qd.shape), X, 0, 0, tiled=True)
    dkv = (dkv[0] + other.astype(jnp.float32)).astype(jnp.bfloat16)
    dkv, od = lax.optimization_barrier((dkv, od))
    dkv = lax.all_to_all(dkv, X, 0, 0, tiled=True)
    half = od.shape[2] // 2
    return (
        by_row(od[:, :, :half]),
        by_row(od[:, :, half:]),
        by_row(dkv[:, :, :HEAD]),
        by_row(dkv[:, :, HEAD:]),
    )


def solution(mesh):
    finer = Mesh(mesh.devices.reshape(mesh.shape["dp"], 4, 4, 2), DP_CTX)
    rows = P(DP_CTX, None)
    return jax.shard_map(
        body,
        mesh=finer,
        in_specs=(P("dp"), P("dp"), rows, rows, rows, rows),
        out_specs=(rows, rows, rows, rows),
        check_vma=False,
    )
```

```python
import functools
import math

import jax
import jax.numpy as jnp
from jax import lax
from jax.experimental import pallas as pl
from jax.experimental.pallas import tpu as pltpu
from jax.sharding import Mesh
from jax.sharding import PartitionSpec as P

BLK = 32
HEAD = 128
TILE = 256
MOST = 1024
LAG = (MOST // BLK + 1 + TILE // BLK - 2) // (TILE // BLK) + 1
RING = LAG + 1
NEG = -1e30


def attend(*refs, docs, slots, group, xs, ys, zs):
    assign_ref, len_ref, coord_ref, qd_in = refs[:4]
    kv_in, od_out, dkv_out = refs[4:4 + ys], refs[4 + ys], refs[5 + ys:5 + 2 * ys]
    (qd, kv, od, dkv, dk, dv, ot, dqt, e_scr, dp_scr, tile_top, top_s, sum_s, del_s, from_s, place_s,
     unit_block, unit_tile, qd_sem, kv_sem, od_sem, dkv_sem) = refs[5 + 2 * ys:]
    scale = HEAD ** -0.5
    steep = scale * math.log2(math.e)
    per = slots // (xs * ys * zs)
    blocks = xs * per
    rows = group * BLK
    tiles = slots * BLK // TILE
    tile_blocks = TILE // BLK
    NT = (((1,), (1,)), ((), ()))
    NN = (((1,), (0,)), ((), ()))
    dot = functools.partial(lax.dot_general, preferred_element_type=jnp.float32)

    y = coord_ref[0] // zs

    def each_block(k, act):
        def one(n, carry):
            c, j = n // per, n % per
            owner = (c // zs * ys + lax.rem(y + k, ys)) * zs + c % zs
            act(assign_ref[owner * per + j], c, j)
            return carry

        lax.fori_loop(0, slots // ys, one, 0, unroll=8)

    for k in range(ys):
        each_block(
            (ys - k) % ys,
            lambda b, c, j: pltpu.make_async_copy(kv_in[k].at[c, :, j], kv.at[b], kv_sem).start(),
        )
    qd_copy = pltpu.make_async_copy(qd_in, qd, qd_sem)
    qd_copy.start()

    for n in range(LAG):
        unit_block[n] = blocks
        unit_tile[n] = 0
    lane = lax.broadcasted_iota(jnp.int32, (1, rows), 1) % BLK

    def plan(i, n):
        slot = ((i // per) * (ys * zs) + coord_ref[0]) * per + i % per
        first = assign_ref[slot] * BLK
        place = first + lane
        from_row = jnp.zeros((1, rows), jnp.int32)
        start = jnp.int32(0)
        bound = jnp.int32(0)
        for d in range(docs):
            bound = bound + len_ref[d]
            from_row = jnp.where(place >= bound, bound, from_row)
            start = jnp.where(first >= bound, bound, start)
        from_s[i] = from_row
        place_s[i] = place
        top_s[i] = jnp.full((1, rows), NEG, jnp.float32)
        sum_s[i] = jnp.zeros((1, rows), jnp.float32)
        del_s[i] = jnp.zeros((1, rows), jnp.float32)
        ot[i] = jnp.zeros((HEAD, rows), jnp.float32)
        dqt[i] = jnp.zeros((HEAD, rows), jnp.float32)

        def unit(t, n):
            unit_block[n] = i
            unit_tile[n] = t
            return n + 1

        return lax.fori_loop(start // TILE, (first + BLK - 1) // TILE + 1, unit, n)

    units = lax.fori_loop(0, blocks, plan, jnp.int32(LAG))
    for n in range(LAG):
        unit_block[units + n] = blocks
        unit_tile[units + n] = 0
    for n in range(RING):
        e_scr[n] = jnp.zeros((TILE, rows), jnp.float32)
        dp_scr[n] = jnp.zeros((TILE, rows), jnp.float32)
        tile_top[n] = jnp.zeros((1, rows), jnp.float32)
    from_s[blocks] = jnp.zeros((1, rows), jnp.int32)
    place_s[blocks] = jnp.zeros((1, rows), jnp.int32)
    top_s[blocks] = jnp.zeros((1, rows), jnp.float32)
    sum_s[blocks] = jnp.ones((1, rows), jnp.float32)
    del_s[blocks] = jnp.zeros((1, rows), jnp.float32)
    ot[blocks] = jnp.zeros((HEAD, rows), jnp.float32)
    dqt[blocks] = jnp.zeros((HEAD, rows), jnp.float32)

    def clear(t, carry):
        dk[t] = jnp.zeros((TILE, HEAD), jnp.float32)
        dv[t] = jnp.zeros((TILE, HEAD), jnp.float32)
        return carry

    lax.fori_loop(0, tiles, clear, 0)
    pltpu.make_async_copy(kv, kv, kv_sem).wait()

    def keys(t):
        return kv[pl.ds(t * tile_blocks, tile_blocks), 0].reshape(TILE, HEAD)

    def values(t):
        return kv[pl.ds(t * tile_blocks, tile_blocks), 1].reshape(TILE, HEAD)

    key = lax.broadcasted_iota(jnp.int32, (TILE, rows), 0)

    def rows_of(i, which):
        i = jnp.minimum(i, blocks - 1)
        return qd[i // per, which, i % per].reshape(rows, HEAD)

    qd_copy.wait()

    def step(u, carry):
        old = unit_block[u]
        t = unit_tile[u]
        spot = lax.rem(u + RING - LAG, RING)
        total = 1.0 / sum_s[old]
        weight = jnp.exp2((tile_top[spot] - top_s[old]) * steep) * total
        delta = del_s[old] * total
        p = e_scr[spot] * weight
        pb = p.astype(jnp.bfloat16)
        ds = (p * (dp_scr[spot] - delta)).astype(jnp.bfloat16)
        ot[old] += dot(values(t).T, pb, NN)
        dqt[old] += dot(keys(t).T, ds, NN)
        dv[t] += dot(pb, rows_of(old, 1), NN)
        dk[t] += dot(ds, rows_of(old, 0), NN)

        i = unit_block[u + LAG]
        t = unit_tile[u + LAG]
        spot = lax.rem(u, RING)
        s = dot(keys(t), rows_of(i, 0), NT)
        dp = dot(values(t), rows_of(i, 1), NT)
        s = jnp.where((key >= from_s[i] - t * TILE) & (key <= place_s[i] - t * TILE), s, NEG)
        top = jnp.max(jnp.max(s.reshape(TILE // 8, 8, rows), axis=0), axis=0, keepdims=True)
        e = jnp.exp2((s - top) * steep)
        e_scr[spot] = e
        dp_scr[spot] = dp
        tile_top[spot] = top
        tile_sum = jnp.sum(jnp.sum(e.reshape(TILE // 8, 8, rows), axis=0), axis=0, keepdims=True)
        tile_del = jnp.sum(jnp.sum((e * dp).reshape(TILE // 8, 8, rows), axis=0), axis=0, keepdims=True)
        was = top_s[i]
        now = jnp.maximum(was, top)
        keep = jnp.exp2((was - now) * steep)
        take = jnp.exp2((top - now) * steep)
        top_s[i] = now
        sum_s[i] = sum_s[i] * keep + tile_sum * take
        del_s[i] = del_s[i] * keep + tile_del * take
        return carry

    lax.fori_loop(0, units, step, 0)

    def gone(t, carry):
        at = pl.ds(t * tile_blocks, tile_blocks)
        dkv[at, 0] = (dk[t] * scale).astype(jnp.bfloat16).reshape(tile_blocks, BLK, HEAD)
        dkv[at, 1] = dv[t].astype(jnp.bfloat16).reshape(tile_blocks, BLK, HEAD)
        return carry

    lax.fori_loop(0, tiles, gone, 0, unroll=2)
    for k in range(ys):
        each_block(
            k, lambda b, c, j: pltpu.make_async_copy(dkv.at[b], dkv_out[k].at[c, :, j], dkv_sem).start()
        )

    def rows_out(i, carry):
        od[i // per, 0, i % per] = ot[i].T.astype(jnp.bfloat16).reshape(group, BLK, HEAD)
        od[i // per, 1, i % per] = (dqt[i].T * scale).astype(jnp.bfloat16).reshape(group, BLK, HEAD)
        return carry

    lax.fori_loop(0, blocks, rows_out, 0, unroll=2)
    od_copy = pltpu.make_async_copy(od, od_out, od_sem)
    od_copy.start()
    pltpu.make_async_copy(dkv, dkv, dkv_sem).wait()
    od_copy.wait()


def attention(assign, lengths, coord, qd, kv, *, xs, ys, zs):
    blocks = qd.shape[0] * qd.shape[2]
    group = qd.shape[3]
    slots = ys * kv[0].shape[0] * kv[0].shape[2]
    tiles = slots * BLK // TILE
    rows = group * BLK
    f32, bf, i32 = jnp.float32, jnp.bfloat16, jnp.int32
    body = functools.partial(attend, docs=lengths.shape[0], slots=slots, group=group, xs=xs, ys=ys, zs=zs)
    smem = pl.BlockSpec(memory_space=pltpu.SMEM)
    anywhere = pl.BlockSpec(memory_space=pl.ANY)
    return pl.pallas_call(
        body,
        out_shape=[jax.ShapeDtypeStruct(a.shape, bf) for a in (qd, *kv)],
        in_specs=[smem] * 3 + [anywhere] * (1 + ys),
        out_specs=[anywhere] * (1 + ys),
        scratch_shapes=[
            pltpu.VMEM(qd.shape, bf), pltpu.VMEM((slots, 2, BLK, HEAD), bf),
            pltpu.VMEM(qd.shape, bf), pltpu.VMEM((slots, 2, BLK, HEAD), bf),
            pltpu.VMEM((tiles, TILE, HEAD), f32), pltpu.VMEM((tiles, TILE, HEAD), f32),
            pltpu.VMEM((blocks + 1, HEAD, rows), f32), pltpu.VMEM((blocks + 1, HEAD, rows), f32),
            pltpu.VMEM((RING, TILE, rows), f32), pltpu.VMEM((RING, TILE, rows), f32),
            pltpu.VMEM((RING, 1, rows), f32),
            pltpu.VMEM((blocks + 1, 1, rows), f32), pltpu.VMEM((blocks + 1, 1, rows), f32),
            pltpu.VMEM((blocks + 1, 1, rows), f32), pltpu.VMEM((blocks + 1, 1, rows), i32),
            pltpu.VMEM((blocks + 1, 1, rows), i32),
            pltpu.SMEM((blocks * LAG + 2 * LAG,), i32), pltpu.SMEM((blocks * LAG + 2 * LAG,), i32),
            pltpu.SemaphoreType.DMA, pltpu.SemaphoreType.DMA, pltpu.SemaphoreType.DMA, pltpu.SemaphoreType.DMA,
        ],
        compiler_params=pltpu.CompilerParams(vmem_limit_bytes=40 << 20),
        cost_estimate=pl.CostEstimate(flops=10 ** 9, bytes_accessed=8 << 20, transcendentals=0),
        name="attend",
    )(assign, lengths, coord, qd, *kv)


def lay_out(a_ref, b_ref, o_ref, *, xs, per, heads, copies):
    for which, ref in enumerate((a_ref, b_ref)):
        for x in range(xs):
            for h in range(heads):
                c = (x * heads + h) * HEAD
                block = ref[:, c:c + HEAD].reshape(per, BLK, HEAD)
                for n in range(copies):
                    if heads == 1:
                        o_ref[x * copies + n, which] = block
                    else:
                        o_ref[x * copies + n, which, :, h] = block


def spread(a, b, xs, copies):
    per = a.shape[0] // BLK
    heads = a.shape[1] // (xs * HEAD)
    shape = (xs * copies, 2, per) + ((heads,) if heads > 1 else ()) + (BLK, HEAD)
    return pl.pallas_call(
        functools.partial(lay_out, xs=xs, per=per, heads=heads, copies=copies),
        out_shape=jax.ShapeDtypeStruct(shape, a.dtype),
        cost_estimate=pl.CostEstimate(flops=10 ** 6, bytes_accessed=4 * a.size, transcendentals=0),
        name="spread",
    )(a, b)


def line_up(a_ref, p_ref, q_ref, *, xs, per, heads, copies):
    for which, ref in enumerate((p_ref, q_ref)):
        for x in range(xs):
            for h in range(heads):
                c = (x * heads + h) * HEAD
                if heads == 1:
                    block = a_ref[x * copies, which].astype(jnp.float32)
                    for n in range(1, copies):
                        block += a_ref[x * copies + n, which].astype(jnp.float32)
                    block = block.astype(jnp.bfloat16)
                else:
                    block = a_ref[x, which, :, h]
                ref[:, c:c + HEAD] = block.reshape(per * BLK, HEAD)


def gather(a, xs):
    copies, per = a.shape[0] // xs, a.shape[2]
    heads = a.shape[3] if a.ndim == 6 else 1
    out = jax.ShapeDtypeStruct((per * BLK, xs * heads * HEAD), a.dtype)
    return pl.pallas_call(
        functools.partial(line_up, xs=xs, per=per, heads=heads, copies=copies),
        out_shape=(out, out),
        cost_estimate=pl.CostEstimate(flops=10 ** 6, bytes_accessed=2 * a.size, transcendentals=0),
        name="gather",
    )(a)


X, Y, Z = "ctx_0", "ctx_1", "ctx_2"
DP_CTX = ("dp", X, Y, Z)


def shift(k, size):
    return [(i, (i + k) % size) for i in range(size)]


def body(doc_lengths, assignment, queries, key_state_rows, value_state_rows, out_grad):
    xs, ys, zs = (lax.axis_size(name) for name in (X, Y, Z))
    coord = lax.axis_index((Y, Z)).reshape(1).astype(jnp.int32)

    kv = spread(key_state_rows, value_state_rows, xs, zs)
    kv = lax.all_to_all(kv, (X, Z), 0, 0, tiled=True)
    qd = spread(queries, out_grad, xs, 1)
    with jax.named_scope("kv_y"):
        kv = [kv] + [lax.ppermute(kv, Y, shift(k, ys)) for k in range(1, ys)]
    with jax.named_scope("qd_x"):
        qd = lax.all_to_all(qd, X, 0, 0, tiled=True)

    od, *dkv = attention(assignment, doc_lengths, coord, qd, kv, xs=xs, ys=ys, zs=zs)

    with jax.named_scope("dkv_y"):
        dkv = dkv[:1] + [lax.ppermute(dkv[k], Y, shift(k, ys)) for k in range(1, ys)]
    with jax.named_scope("od_x"):
        od = lax.all_to_all(od, X, 0, 0, tiled=True)
    dkv = sum(part.astype(jnp.float32) for part in dkv).astype(jnp.bfloat16)
    dkv, od = lax.optimization_barrier((dkv, od))
    dkv = lax.all_to_all(dkv, (X, Z), 0, 0, tiled=True)
    return (*gather(od, xs), *gather(dkv, xs))


def solution(mesh):
    finer = Mesh(mesh.devices.reshape(mesh.shape["dp"], 4, 4, 2), DP_CTX)
    rows = P(DP_CTX, None)
    return jax.shard_map(
        body,
        mesh=finer,
        in_specs=(P("dp"), P("dp"), rows, rows, rows, rows),
        out_specs=(rows, rows, rows, rows),
        check_vma=False,
    )
```

```python
import functools
import math

import jax
import jax.numpy as jnp
from jax import lax
from jax.experimental import pallas as pl
from jax.experimental.pallas import tpu as pltpu
from jax.sharding import Mesh
from jax.sharding import PartitionSpec as P

BLK = 32
HEAD = 128
TILE = 256
MOST = 1024
LAG = (MOST // BLK + 1 + TILE // BLK - 2) // (TILE // BLK) + 1
RING = LAG
NEG = -1e30


def attend(*refs, docs, slots, group, xs, ys, zs):
    assign_ref, len_ref, coord_ref, qd_in = refs[:4]
    parts = ys * zs
    kv_in, od_out, dkv_out = refs[4:4 + parts], refs[4 + parts], refs[5 + parts:5 + 2 * parts]
    (qd, kv, od, dkv, dk, dv, ot, dqt, e_scr, dp_scr, tile_top, top_s, sum_s, del_s, from_s, place_s,
     unit_block, unit_tile, qd_sem, kv_sem, od_sem, dkv_sem) = refs[5 + 2 * parts:]
    scale = HEAD ** -0.5
    steep = scale * math.log2(math.e)
    per = slots // (xs * ys * zs)
    blocks = xs * per
    rows = group * BLK
    tiles = slots * BLK // TILE
    tile_blocks = TILE // BLK
    NT = (((1,), (1,)), ((), ()))
    NN = (((1,), (0,)), ((), ()))
    dot = functools.partial(lax.dot_general, preferred_element_type=jnp.float32)

    y, z = coord_ref[0] // zs, coord_ref[0] % zs

    def each_block(k, w, act):
        base = (lax.rem(y + k, ys) * zs + lax.rem(z + w, zs)) * per
        for x in range(xs):
            for j in range(per):
                act(assign_ref[base + (x * ys * zs * per + j)], x, j)

    for k in range(ys):
        for w in range(zs):
            part = kv_in[k * zs + w]
            each_block(
                (ys - k) % ys,
                w,
                lambda b, x, j: pltpu.make_async_copy(part.at[x, :, j], kv.at[b], kv_sem).start(),
            )
    qd_copy = pltpu.make_async_copy(qd_in, qd, qd_sem)
    qd_copy.start()

    for n in range(LAG):
        unit_block[n] = blocks
        unit_tile[n] = 0
    lane = lax.broadcasted_iota(jnp.int32, (1, rows), 1) % BLK

    def plan(i, n):
        slot = ((i // per) * (ys * zs) + coord_ref[0]) * per + i % per
        first = assign_ref[slot] * BLK
        place = first + lane
        from_row = jnp.zeros((1, rows), jnp.int32)
        start = jnp.int32(0)
        bound = jnp.int32(0)
        for d in range(docs):
            bound = bound + len_ref[d]
            from_row = jnp.where(place >= bound, bound, from_row)
            start = jnp.where(first >= bound, bound, start)
        from_s[i] = from_row
        place_s[i] = place
        top_s[i] = jnp.full((1, rows), NEG, jnp.float32)
        sum_s[i] = jnp.zeros((1, rows), jnp.float32)
        del_s[i] = jnp.zeros((1, rows), jnp.float32)
        ot[i] = jnp.zeros((HEAD, rows), jnp.float32)
        dqt[i] = jnp.zeros((HEAD, rows), jnp.float32)

        def unit(t, n):
            unit_block[n] = i
            unit_tile[n] = t
            return n + 1

        return lax.fori_loop(start // TILE, (first + BLK - 1) // TILE + 1, unit, n)

    units = lax.fori_loop(0, blocks, plan, jnp.int32(LAG))
    for n in range(LAG):
        unit_block[units + n] = blocks
        unit_tile[units + n] = 0
    for n in range(RING):
        e_scr[n] = jnp.zeros((TILE, rows), jnp.float32)
        dp_scr[n] = jnp.zeros((TILE, rows), jnp.float32)
        tile_top[n] = jnp.zeros((1, rows), jnp.float32)
    from_s[blocks] = jnp.zeros((1, rows), jnp.int32)
    place_s[blocks] = jnp.zeros((1, rows), jnp.int32)
    top_s[blocks] = jnp.zeros((1, rows), jnp.float32)
    sum_s[blocks] = jnp.ones((1, rows), jnp.float32)
    del_s[blocks] = jnp.zeros((1, rows), jnp.float32)
    ot[blocks] = jnp.zeros((HEAD, rows), jnp.float32)
    dqt[blocks] = jnp.zeros((HEAD, rows), jnp.float32)

    def clear(t, carry):
        dk[t] = jnp.zeros((TILE, HEAD), jnp.float32)
        dv[t] = jnp.zeros((TILE, HEAD), jnp.float32)
        return carry

    lax.fori_loop(0, tiles, clear, 0)
    pltpu.make_async_copy(kv, kv, kv_sem).wait()

    def keys(t):
        return kv[pl.ds(t * tile_blocks, tile_blocks), 0].reshape(TILE, HEAD)

    def values(t):
        return kv[pl.ds(t * tile_blocks, tile_blocks), 1].reshape(TILE, HEAD)

    key = lax.broadcasted_iota(jnp.int32, (TILE, rows), 0)

    def rows_of(i, which):
        i = jnp.minimum(i, blocks - 1)
        return qd[i // per, which, i % per].reshape(rows, HEAD)

    qd_copy.wait()

    def scores(u, spot):
        i = unit_block[u + LAG]
        t = unit_tile[u + LAG]
        s = dot(keys(t), rows_of(i, 0), NT)
        dp = dot(values(t), rows_of(i, 1), NT)
        s = jnp.where((key >= from_s[i] - t * TILE) & (key <= place_s[i] - t * TILE), s, NEG)
        top = jnp.max(jnp.max(s.reshape(TILE // 8, 8, rows), axis=0), axis=0, keepdims=True)
        e = jnp.exp2((s - top) * steep)
        tile_sum = jnp.sum(jnp.sum(e.reshape(TILE // 8, 8, rows), axis=0), axis=0, keepdims=True)
        tile_del = jnp.sum(jnp.sum((e * dp).reshape(TILE // 8, 8, rows), axis=0), axis=0, keepdims=True)
        e_scr[spot] = e
        dp_scr[spot] = dp
        tile_top[spot] = top
        was = top_s[i]
        now = jnp.maximum(was, top)
        keep = jnp.exp2((was - now) * steep)
        take = jnp.exp2((top - now) * steep)
        top_s[i] = now
        sum_s[i] = sum_s[i] * keep + tile_sum * take
        del_s[i] = del_s[i] * keep + tile_del * take

    def grads(u, spot):
        old = unit_block[u]
        t = unit_tile[u]
        total = 1.0 / sum_s[old]
        weight = jnp.exp2((tile_top[spot] - top_s[old]) * steep) * total
        delta = del_s[old] * total
        p = e_scr[spot] * weight
        pb = p.astype(jnp.bfloat16)
        ds = (p * (dp_scr[spot] - delta)).astype(jnp.bfloat16)
        ot[old] += dot(values(t).T, pb, NN)
        dqt[old] += dot(keys(t).T, ds, NN)
        dv[t] += dot(pb, rows_of(old, 1), NN)
        dk[t] += dot(ds, rows_of(old, 0), NN)

    def step(u, carry):
        spot = lax.rem(u, RING)
        grads(u, spot)
        scores(u, spot)
        return carry

    lax.fori_loop(0, units, step, 0)

    def gone(t, carry):
        at = pl.ds(t * tile_blocks, tile_blocks)
        dkv[at, 0] = (dk[t] * scale).astype(jnp.bfloat16).reshape(tile_blocks, BLK, HEAD)
        dkv[at, 1] = dv[t].astype(jnp.bfloat16).reshape(tile_blocks, BLK, HEAD)
        return carry

    lax.fori_loop(0, tiles, gone, 0, unroll=2)
    for k in range(ys):
        for w in range(zs):
            part = dkv_out[k * zs + w]
            each_block(
                k, w, lambda b, x, j: pltpu.make_async_copy(dkv.at[b], part.at[x, :, j], dkv_sem).start()
            )

    def rows_out(i, carry):
        od[i // per, 0, i % per] = ot[i].T.astype(jnp.bfloat16).reshape(group, BLK, HEAD)
        od[i // per, 1, i % per] = (dqt[i].T * scale).astype(jnp.bfloat16).reshape(group, BLK, HEAD)
        return carry

    lax.fori_loop(0, blocks, rows_out, 0, unroll=2)
    od_copy = pltpu.make_async_copy(od, od_out, od_sem)
    od_copy.start()
    pltpu.make_async_copy(dkv, dkv, dkv_sem).wait()
    od_copy.wait()


def attention(assign, lengths, coord, qd, kv, *, xs, ys, zs):
    blocks = qd.shape[0] * qd.shape[2]
    group = qd.shape[3]
    slots = len(kv) * kv[0].shape[0] * kv[0].shape[2]
    tiles = slots * BLK // TILE
    rows = group * BLK
    f32, bf, i32 = jnp.float32, jnp.bfloat16, jnp.int32
    body = functools.partial(attend, docs=lengths.shape[0], slots=slots, group=group, xs=xs, ys=ys, zs=zs)
    smem = pl.BlockSpec(memory_space=pltpu.SMEM)
    far = pl.BlockSpec(memory_space=pltpu.HBM)
    return pl.pallas_call(
        body,
        out_shape=[jax.ShapeDtypeStruct(a.shape, bf) for a in (qd, *kv)],
        in_specs=[smem] * 3 + [far] * (1 + len(kv)),
        out_specs=[far] * (1 + len(kv)),
        scratch_shapes=[
            pltpu.VMEM(qd.shape, bf), pltpu.VMEM((slots, 2, BLK, HEAD), bf),
            pltpu.VMEM(qd.shape, bf), pltpu.VMEM((slots, 2, BLK, HEAD), bf),
            pltpu.VMEM((tiles, TILE, HEAD), f32), pltpu.VMEM((tiles, TILE, HEAD), f32),
            pltpu.VMEM((blocks + 1, HEAD, rows), f32), pltpu.VMEM((blocks + 1, HEAD, rows), f32),
            pltpu.VMEM((RING, TILE, rows), f32), pltpu.VMEM((RING, TILE, rows), f32),
            pltpu.VMEM((RING, 1, rows), f32),
            pltpu.VMEM((blocks + 1, 1, rows), f32), pltpu.VMEM((blocks + 1, 1, rows), f32),
            pltpu.VMEM((blocks + 1, 1, rows), f32), pltpu.VMEM((blocks + 1, 1, rows), i32),
            pltpu.VMEM((blocks + 1, 1, rows), i32),
            pltpu.SMEM((blocks * LAG + 2 * LAG,), i32), pltpu.SMEM((blocks * LAG + 2 * LAG,), i32),
            pltpu.SemaphoreType.DMA, pltpu.SemaphoreType.DMA, pltpu.SemaphoreType.DMA, pltpu.SemaphoreType.DMA,
        ],
        compiler_params=pltpu.CompilerParams(vmem_limit_bytes=63 << 20),
        cost_estimate=pl.CostEstimate(flops=10 ** 9, bytes_accessed=8 << 20, transcendentals=0),
        name="attend",
    )(assign, lengths, coord, qd, *kv)


def lay_out(a_ref, b_ref, o_ref, *, xs, per, heads, copies):
    for which, ref in enumerate((a_ref, b_ref)):
        for x in range(xs):
            for h in range(heads):
                c = (x * heads + h) * HEAD
                block = ref[:, c:c + HEAD].reshape(per, BLK, HEAD)
                for n in range(copies):
                    if heads == 1:
                        o_ref[x * copies + n, which] = block
                    else:
                        o_ref[x * copies + n, which, :, h] = block


def spread(a, b, xs, copies):
    per = a.shape[0] // BLK
    heads = a.shape[1] // (xs * HEAD)
    shape = (xs * copies, 2, per) + ((heads,) if heads > 1 else ()) + (BLK, HEAD)
    return pl.pallas_call(
        functools.partial(lay_out, xs=xs, per=per, heads=heads, copies=copies),
        out_shape=jax.ShapeDtypeStruct(shape, a.dtype),
        cost_estimate=pl.CostEstimate(flops=10 ** 6, bytes_accessed=4 * a.size, transcendentals=0),
        name="spread",
    )(a, b)


def line_up(a_ref, p_ref, q_ref, *, xs, per, heads, copies):
    for which, ref in enumerate((p_ref, q_ref)):
        for x in range(xs):
            for h in range(heads):
                c = (x * heads + h) * HEAD
                if heads == 1:
                    block = a_ref[x * copies, which].astype(jnp.float32)
                    for n in range(1, copies):
                        block += a_ref[x * copies + n, which].astype(jnp.float32)
                    block = block.astype(jnp.bfloat16)
                else:
                    block = a_ref[x, which, :, h]
                ref[:, c:c + HEAD] = block.reshape(per * BLK, HEAD)


def gather(a, xs):
    copies, per = a.shape[0] // xs, a.shape[2]
    heads = a.shape[3] if a.ndim == 6 else 1
    out = jax.ShapeDtypeStruct((per * BLK, xs * heads * HEAD), a.dtype)
    return pl.pallas_call(
        functools.partial(line_up, xs=xs, per=per, heads=heads, copies=copies),
        out_shape=(out, out),
        cost_estimate=pl.CostEstimate(flops=10 ** 6, bytes_accessed=2 * a.size, transcendentals=0),
        compiler_params=pltpu.CompilerParams(vmem_limit_bytes=16 << 20),
        name="gather",
    )(a)


X, Y, Z = "ctx_0", "ctx_1", "ctx_2"
DP_CTX = ("dp", X, Y, Z)


def shift(k, size):
    return [(i, (i + k) % size) for i in range(size)]


def body(doc_lengths, assignment, queries, key_state_rows, value_state_rows, out_grad):
    xs, ys, zs = (lax.axis_size(name) for name in (X, Y, Z))
    coord = lax.axis_index((Y, Z)).reshape(1).astype(jnp.int32)

    kv = spread(key_state_rows, value_state_rows, xs, 1)
    kv = lax.all_to_all(kv, X, 0, 0, tiled=True)
    qd = spread(queries, out_grad, xs, 1)
    kv = [kv] + [lax.ppermute(kv, Z, shift(w, zs)) for w in range(1, zs)]
    kv = [part if k == 0 else lax.ppermute(part, Y, shift(k, ys)) for k in range(ys) for part in kv]
    qd = lax.all_to_all(qd, X, 0, 0, tiled=True)

    od, *dkv = attention(assignment, doc_lengths, coord, qd, kv, xs=xs, ys=ys, zs=zs)

    def over_y(w):
        terms = [dkv[w]] + [lax.ppermute(dkv[k * zs + w], Y, shift(k, ys)) for k in range(1, ys)]
        return sum(part.astype(jnp.float32) for part in terms)

    other = [lax.ppermute(over_y(w).astype(jnp.bfloat16), Z, shift(w, zs)) for w in range(1, zs)]
    od = lax.all_to_all(od, X, 0, 0, tiled=True)
    dkv = sum([part.astype(jnp.float32) for part in other], over_y(0)).astype(jnp.bfloat16)
    dkv, od = lax.optimization_barrier((dkv, od))
    dkv = lax.all_to_all(dkv, X, 0, 0, tiled=True)
    return (*gather(od, xs), *gather(dkv, xs))


def solution(mesh):
    finer = Mesh(mesh.devices.reshape(mesh.shape["dp"], 4, 4, 2), DP_CTX)
    rows = P(DP_CTX, None)
    return jax.shard_map(
        body,
        mesh=finer,
        in_specs=(P("dp"), P("dp"), rows, rows, rows, rows),
        out_specs=(rows, rows, rows, rows),
        check_vma=False,
    )
```

```python
import functools
import math

import jax
import jax.numpy as jnp
from jax import lax
from jax.experimental import pallas as pl
from jax.experimental.pallas import tpu as pltpu
from jax.sharding import Mesh
from jax.sharding import PartitionSpec as P

BLK = 32
HEAD = 128
TILE = 256
MOST = 1024
SPAN = (MOST // BLK + 1 + TILE // BLK - 2) // (TILE // BLK) + 1
MANY = 4
LAG = SPAN + MANY - 1
RING = LAG
NEG = -1e30


def attend(*refs, docs, slots, group, xs, ys, zs):
    assign_ref, len_ref, coord_ref, qd_in = refs[:4]
    parts = ys * zs
    kv_in, od_out, dkv_out = refs[4:4 + parts], refs[4 + parts], refs[5 + parts:5 + 2 * parts]
    (qd, kv, od, dkv, dk, dv, ot, dqt, e_scr, dp_scr, tile_top, top_s, sum_s, del_s, from_s, place_s,
     unit_block, unit_tile, qd_sem, kv_sem, od_sem, dkv_sem) = refs[5 + 2 * parts:]
    scale = HEAD ** -0.5
    steep = scale * math.log2(math.e)
    per = slots // (xs * ys * zs)
    blocks = xs * per
    rows = group * BLK
    tiles = slots * BLK // TILE
    tile_blocks = TILE // BLK
    NT = (((1,), (1,)), ((), ()))
    NN = (((1,), (0,)), ((), ()))
    dot = functools.partial(lax.dot_general, preferred_element_type=jnp.float32)

    y, z = coord_ref[0] // zs, coord_ref[0] % zs

    def each_block(k, w, act):
        base = (lax.rem(y + k, ys) * zs + lax.rem(z + w, zs)) * per
        for x in range(xs):
            for j in range(per):
                act(assign_ref[base + (x * ys * zs * per + j)], x, j)

    for k in range(ys):
        for w in range(zs):
            part = kv_in[k * zs + w]
            each_block(
                (ys - k) % ys,
                w,
                lambda b, x, j: pltpu.make_async_copy(part.at[x, :, j], kv.at[b], kv_sem).start(),
            )
    qd_copy = pltpu.make_async_copy(qd_in, qd, qd_sem)
    qd_copy.start()

    lane = lax.broadcasted_iota(jnp.int32, (1, rows), 1) % BLK

    def plan(i, n):
        slot = ((i // per) * (ys * zs) + coord_ref[0]) * per + i % per
        first = assign_ref[slot] * BLK
        place = first + lane
        from_row = jnp.zeros((1, rows), jnp.int32)
        start = jnp.int32(0)
        bound = jnp.int32(0)
        for d in range(docs):
            bound = bound + len_ref[d]
            from_row = jnp.where(place >= bound, bound, from_row)
            start = jnp.where(first >= bound, bound, start)
        from_s[i] = from_row
        place_s[i] = place
        top_s[i] = jnp.full((1, rows), NEG, jnp.float32)
        sum_s[i] = jnp.zeros((1, rows), jnp.float32)
        del_s[i] = jnp.zeros((1, rows), jnp.float32)
        ot[i] = jnp.zeros((HEAD, rows), jnp.float32)
        dqt[i] = jnp.zeros((HEAD, rows), jnp.float32)

        def unit(t, n):
            unit_block[n] = i
            unit_tile[n] = t
            return n + 1

        return lax.fori_loop(start // TILE, (first + BLK - 1) // TILE + 1, unit, n)

    units = lax.fori_loop(0, blocks, plan, jnp.int32(0))

    def clear(t, carry):
        dk[t] = jnp.zeros((TILE, HEAD), jnp.float32)
        dv[t] = jnp.zeros((TILE, HEAD), jnp.float32)
        return carry

    lax.fori_loop(0, tiles, clear, 0)
    pltpu.make_async_copy(kv, kv, kv_sem).wait()

    def keys(t):
        return kv[pl.ds(t * tile_blocks, tile_blocks), 0].reshape(TILE, HEAD)

    def values(t):
        return kv[pl.ds(t * tile_blocks, tile_blocks), 1].reshape(TILE, HEAD)

    key = lax.broadcasted_iota(jnp.int32, (TILE, rows), 0)

    def rows_of(i, which):
        return qd[i // per, which, i % per].reshape(rows, HEAD)

    qd_copy.wait()

    def scores(u, spot):
        i = unit_block[u]
        t = unit_tile[u]
        s = dot(keys(t), rows_of(i, 0), NT)
        dp = dot(values(t), rows_of(i, 1), NT)
        s = jnp.where((key >= from_s[i] - t * TILE) & (key <= place_s[i] - t * TILE), s, NEG)
        top = jnp.max(jnp.max(s.reshape(TILE // 8, 8, rows), axis=0), axis=0, keepdims=True)
        e = jnp.exp2((s - top) * steep)
        tile_sum = jnp.sum(jnp.sum(e.reshape(TILE // 8, 8, rows), axis=0), axis=0, keepdims=True)
        tile_del = jnp.sum(jnp.sum((e * dp).reshape(TILE // 8, 8, rows), axis=0), axis=0, keepdims=True)
        e_scr[spot] = e
        dp_scr[spot] = dp
        tile_top[spot] = top
        was = top_s[i]
        now = jnp.maximum(was, top)
        keep = jnp.exp2((was - now) * steep)
        take = jnp.exp2((top - now) * steep)
        top_s[i] = now
        sum_s[i] = sum_s[i] * keep + tile_sum * take
        del_s[i] = del_s[i] * keep + tile_del * take

    def grads(u, spot):
        old = unit_block[u]
        t = unit_tile[u]
        total = 1.0 / sum_s[old]
        weight = jnp.exp2((tile_top[spot] - top_s[old]) * steep) * total
        delta = del_s[old] * total
        p = e_scr[spot] * weight
        pb = p.astype(jnp.bfloat16)
        ds = (p * (dp_scr[spot] - delta)).astype(jnp.bfloat16)
        ot[old] += dot(values(t).T, pb, NN)
        dqt[old] += dot(keys(t).T, ds, NN)
        dv[t] += dot(pb, rows_of(old, 1), NN)
        dk[t] += dot(ds, rows_of(old, 0), NN)

    def first(u, carry):
        scores(u, u)
        return carry

    def both(u, carry):
        spot = lax.rem(u, RING)
        grads(u - LAG, spot)
        scores(u, spot)
        return carry

    def last(n, carry):
        u = units + n
        grads(u - LAG, lax.rem(u, RING))
        return carry

    def several(n, carry):
        u = LAG + odd + MANY * n
        for m in range(MANY):
            grads(u + m - LAG, lax.rem(u + m, RING))
        for m in range(MANY):
            scores(u + m, lax.rem(u + m, RING))
        return carry

    odd = lax.rem(units - LAG, MANY)
    lax.fori_loop(0, LAG, first, 0, unroll=LAG)
    lax.fori_loop(LAG, LAG + odd, both, 0)
    lax.fori_loop(0, (units - LAG) // MANY, several, 0)
    lax.fori_loop(0, LAG, last, 0, unroll=LAG)

    def gone(t, carry):
        at = pl.ds(t * tile_blocks, tile_blocks)
        dkv[at, 0] = (dk[t] * scale).astype(jnp.bfloat16).reshape(tile_blocks, BLK, HEAD)
        dkv[at, 1] = dv[t].astype(jnp.bfloat16).reshape(tile_blocks, BLK, HEAD)
        return carry

    lax.fori_loop(0, tiles, gone, 0, unroll=2)
    for k in range(ys):
        for w in range(zs):
            part = dkv_out[k * zs + w]
            each_block(
                k, w, lambda b, x, j: pltpu.make_async_copy(dkv.at[b], part.at[x, :, j], dkv_sem).start()
            )

    def rows_out(i, carry):
        od[i // per, 0, i % per] = ot[i].T.astype(jnp.bfloat16).reshape(group, BLK, HEAD)
        od[i // per, 1, i % per] = (dqt[i].T * scale).astype(jnp.bfloat16).reshape(group, BLK, HEAD)
        pltpu.make_async_copy(od.at[i // per, :, i % per], od_out.at[i // per, :, i % per], od_sem).start()
        return carry

    lax.fori_loop(0, blocks, rows_out, 0, unroll=2)
    pltpu.make_async_copy(dkv, dkv, dkv_sem).wait()
    pltpu.make_async_copy(od, od, od_sem).wait()


def attention(assign, lengths, coord, qd, kv, *, xs, ys, zs):
    blocks = qd.shape[0] * qd.shape[2]
    group = qd.shape[3]
    slots = len(kv) * kv[0].shape[0] * kv[0].shape[2]
    tiles = slots * BLK // TILE
    rows = group * BLK
    f32, bf, i32 = jnp.float32, jnp.bfloat16, jnp.int32
    body = functools.partial(attend, docs=lengths.shape[0], slots=slots, group=group, xs=xs, ys=ys, zs=zs)
    smem = pl.BlockSpec(memory_space=pltpu.SMEM)
    far = pl.BlockSpec(memory_space=pltpu.HBM)
    return pl.pallas_call(
        body,
        out_shape=[jax.ShapeDtypeStruct(a.shape, bf) for a in (qd, *kv)],
        in_specs=[smem] * 3 + [far] * (1 + len(kv)),
        out_specs=[far] * (1 + len(kv)),
        scratch_shapes=[
            pltpu.VMEM(qd.shape, bf), pltpu.VMEM((slots, 2, BLK, HEAD), bf),
            pltpu.VMEM(qd.shape, bf), pltpu.VMEM((slots, 2, BLK, HEAD), bf),
            pltpu.VMEM((tiles, TILE, HEAD), f32), pltpu.VMEM((tiles, TILE, HEAD), f32),
            pltpu.VMEM((blocks, HEAD, rows), f32), pltpu.VMEM((blocks, HEAD, rows), f32),
            pltpu.VMEM((RING, TILE, rows), f32), pltpu.VMEM((RING, TILE, rows), f32),
            pltpu.VMEM((RING, 1, rows), f32),
            pltpu.VMEM((blocks, 1, rows), f32), pltpu.VMEM((blocks, 1, rows), f32),
            pltpu.VMEM((blocks, 1, rows), f32), pltpu.VMEM((blocks, 1, rows), i32),
            pltpu.VMEM((blocks, 1, rows), i32),
            pltpu.SMEM((blocks * SPAN,), i32), pltpu.SMEM((blocks * SPAN,), i32),
            pltpu.SemaphoreType.DMA, pltpu.SemaphoreType.DMA, pltpu.SemaphoreType.DMA, pltpu.SemaphoreType.DMA,
        ],
        compiler_params=pltpu.CompilerParams(vmem_limit_bytes=63 << 20),
        cost_estimate=pl.CostEstimate(flops=10 ** 9, bytes_accessed=8 << 20, transcendentals=0),
        name="attend",
    )(assign, lengths, coord, qd, *kv)


def lay_out(a_ref, b_ref, o_ref, *, xs, per, heads, copies):
    for which, ref in enumerate((a_ref, b_ref)):
        for x in range(xs):
            for h in range(heads):
                c = (x * heads + h) * HEAD
                block = ref[:, c:c + HEAD].reshape(per, BLK, HEAD)
                for n in range(copies):
                    if heads == 1:
                        o_ref[x * copies + n, which] = block
                    else:
                        o_ref[x * copies + n, which, :, h] = block


def spread(a, b, xs, copies):
    per = a.shape[0] // BLK
    heads = a.shape[1] // (xs * HEAD)
    shape = (xs * copies, 2, per) + ((heads,) if heads > 1 else ()) + (BLK, HEAD)
    return pl.pallas_call(
        functools.partial(lay_out, xs=xs, per=per, heads=heads, copies=copies),
        out_shape=jax.ShapeDtypeStruct(shape, a.dtype),
        cost_estimate=pl.CostEstimate(flops=10 ** 6, bytes_accessed=4 * a.size, transcendentals=0),
        name="spread",
    )(a, b)


def line_up(a_ref, p_ref, q_ref, *, xs, per, heads, copies):
    for which, ref in enumerate((p_ref, q_ref)):
        for x in range(xs):
            for h in range(heads):
                c = (x * heads + h) * HEAD
                if heads == 1:
                    block = a_ref[x * copies, which].astype(jnp.float32)
                    for n in range(1, copies):
                        block += a_ref[x * copies + n, which].astype(jnp.float32)
                    block = block.astype(jnp.bfloat16)
                else:
                    block = a_ref[x, which, :, h]
                ref[:, c:c + HEAD] = block.reshape(per * BLK, HEAD)


def gather(a, xs):
    copies, per = a.shape[0] // xs, a.shape[2]
    heads = a.shape[3] if a.ndim == 6 else 1
    out = jax.ShapeDtypeStruct((per * BLK, xs * heads * HEAD), a.dtype)
    return pl.pallas_call(
        functools.partial(line_up, xs=xs, per=per, heads=heads, copies=copies),
        out_shape=(out, out),
        cost_estimate=pl.CostEstimate(flops=10 ** 6, bytes_accessed=2 * a.size, transcendentals=0),
        compiler_params=pltpu.CompilerParams(vmem_limit_bytes=16 << 20),
        name="gather",
    )(a)


X, Y, Z = "ctx_0", "ctx_1", "ctx_2"
DP_CTX = ("dp", X, Y, Z)


def shift(k, size):
    return [(i, (i + k) % size) for i in range(size)]


def work(doc_lengths, assignment, queries, key_state_rows, value_state_rows, out_grad):
    xs, ys, zs = (lax.axis_size(name) for name in (X, Y, Z))
    coord = lax.axis_index((Y, Z)).reshape(1).astype(jnp.int32)

    kv = spread(key_state_rows, value_state_rows, xs, 1)
    kv = lax.all_to_all(kv, X, 0, 0, tiled=True)
    qd = spread(queries, out_grad, xs, 1)
    kv = [kv] + [lax.ppermute(kv, Z, shift(w, zs)) for w in range(1, zs)]
    parts = [kv]
    for k in range(1, ys):
        own = lax.ppermute(kv[0], Y, shift(k, ys))
        parts.append([own] + [lax.ppermute(part, Y, shift(k, ys)) for part in kv[1:]])
    kv = [part for row in parts for part in row]
    qd = lax.all_to_all(qd, X, 0, 0, tiled=True)

    od, *dkv = attention(assignment, doc_lengths, coord, qd, kv, xs=xs, ys=ys, zs=zs)

    def over_y(w):
        terms = [dkv[w]]
        for k in range(1, ys):
            terms.append(lax.ppermute(dkv[k * zs + w], Y, shift(k, ys)))
        return sum(part.astype(jnp.float32) for part in terms)

    other = [lax.ppermute(over_y(w).astype(jnp.bfloat16), Z, shift(w, zs)) for w in range(1, zs)]
    od = lax.all_to_all(od, X, 0, 0, tiled=True)
    dkv = sum([part.astype(jnp.float32) for part in other], over_y(0)).astype(jnp.bfloat16)
    dkv, od = lax.optimization_barrier((dkv, od))
    dkv = lax.all_to_all(dkv, X, 0, 0, tiled=True)
    return (*gather(od, xs), *gather(dkv, xs))


def solution(mesh):
    finer = Mesh(mesh.devices.reshape(mesh.shape["dp"], 4, 4, 2), DP_CTX)
    rows = P(DP_CTX, None)
    return jax.shard_map(
        work,
        mesh=finer,
        in_specs=(P("dp"), P("dp"), rows, rows, rows, rows),
        out_specs=(rows, rows, rows, rows),
        check_vma=False,
    )
```

```python
import functools
import math

import jax
import jax.numpy as jnp
from jax import lax
from jax.experimental import pallas as pl
from jax.experimental.pallas import tpu as pltpu
from jax.sharding import Mesh
from jax.sharding import PartitionSpec as P

BLK = 32
HEAD = 128
TILE = 256
MOST = 1024
SPAN = MOST // TILE + 1
PAD = TILE // BLK
MANY = 4
LAG = SPAN + MANY - 1
RING = LAG
NEG = -1e30


def attend(*refs, docs, slots, group, xs, ys, zs):
    assign_ref, len_ref, coord_ref, qd_in = refs[:4]
    parts = ys * zs
    kv_in, od_out, dkv_out = refs[4:4 + parts], refs[4 + parts], refs[5 + parts:5 + 2 * parts]
    (qd, kv, od, dkv, dk, dv, ot, dqt, e_scr, dp_scr, tile_top, top_s, sum_s, del_s, from_s, place_s,
     unit_block, unit_tile, qd_sem, kv_sem, od_sem, dkv_sem) = refs[5 + 2 * parts:]
    scale = HEAD ** -0.5
    steep = scale * math.log2(math.e)
    per = slots // (xs * ys * zs)
    blocks = xs * per
    rows = group * BLK
    tiles = slots * BLK // TILE
    tile_blocks = TILE // BLK
    NT = (((1,), (1,)), ((), ()))
    NN = (((1,), (0,)), ((), ()))
    dot = functools.partial(lax.dot_general, preferred_element_type=jnp.float32)

    y, z = coord_ref[0] // zs, coord_ref[0] % zs

    def each_block(k, w, act):
        base = (lax.rem(y + k, ys) * zs + lax.rem(z + w, zs)) * per
        for x in range(xs):
            for j in range(per):
                act(assign_ref[base + (x * ys * zs * per + j)], x, j)

    for k in range(ys):
        for w in range(zs):
            part = kv_in[k * zs + w]
            each_block(
                (ys - k) % ys,
                w,
                lambda b, x, j: pltpu.make_async_copy(part.at[x, :, j], kv.at[PAD + b], kv_sem).start(),
            )
    qd_copy = pltpu.make_async_copy(qd_in, qd, qd_sem)
    qd_copy.start()

    lane = lax.broadcasted_iota(jnp.int32, (1, rows), 1) % BLK

    def plan(i, n):
        slot = ((i // per) * (ys * zs) + coord_ref[0]) * per + i % per
        first = assign_ref[slot] * BLK
        place = first + lane
        from_row = jnp.zeros((1, rows), jnp.int32)
        start = jnp.int32(0)
        bound = jnp.int32(0)
        for d in range(docs):
            bound = bound + len_ref[d]
            from_row = jnp.where(place >= bound, bound, from_row)
            start = jnp.where(first >= bound, bound, start)
        from_s[i] = from_row
        place_s[i] = place
        top_s[i] = jnp.full((1, rows), NEG, jnp.float32)
        sum_s[i] = jnp.zeros((1, rows), jnp.float32)
        del_s[i] = jnp.zeros((1, rows), jnp.float32)
        ot[i] = jnp.zeros((HEAD, rows), jnp.float32)
        dqt[i] = jnp.zeros((HEAD, rows), jnp.float32)

        def unit(t, n):
            unit_block[n] = i
            unit_tile[n] = first // BLK + 1 - t * tile_blocks
            return n + 1

        return lax.fori_loop(0, (first // BLK - start // BLK) // tile_blocks + 1, unit, n)

    units = lax.fori_loop(0, blocks, plan, jnp.int32(0))

    nought = jnp.zeros((tile_blocks, BLK, HEAD), jnp.float32)
    kv[:PAD] = jnp.zeros((PAD, 2, BLK, HEAD), jnp.bfloat16)

    def clear(t, carry):
        dk[pl.ds(t * tile_blocks, tile_blocks)] = nought
        dv[pl.ds(t * tile_blocks, tile_blocks)] = nought
        return carry

    lax.fori_loop(0, tiles + 1, clear, 0)
    pltpu.make_async_copy(kv.at[pl.ds(PAD, slots)], kv.at[pl.ds(PAD, slots)], kv_sem).wait()

    def keys(t):
        return kv[pl.ds(t, tile_blocks), 0].reshape(TILE, HEAD)

    def values(t):
        return kv[pl.ds(t, tile_blocks), 1].reshape(TILE, HEAD)

    key = lax.broadcasted_iota(jnp.int32, (TILE, rows), 0)

    def rows_of(i, which):
        return qd[i // per, which, i % per].reshape(rows, HEAD)

    qd_copy.wait()

    def scores(u, spot):
        i = unit_block[u]
        t = unit_tile[u]
        s = dot(keys(t), rows_of(i, 0), NT)
        dp = dot(values(t), rows_of(i, 1), NT)
        ahead = (t - PAD) * BLK
        s = jnp.where((key >= from_s[i] - ahead) & (key <= place_s[i] - ahead), s, NEG)
        top = jnp.max(jnp.max(s.reshape(TILE // 8, 8, rows), axis=0), axis=0, keepdims=True)
        e = jnp.exp2((s - top) * steep)
        tile_sum = jnp.sum(jnp.sum(e.reshape(TILE // 8, 8, rows), axis=0), axis=0, keepdims=True)
        tile_del = jnp.sum(jnp.sum((e * dp).reshape(TILE // 8, 8, rows), axis=0), axis=0, keepdims=True)
        e_scr[spot] = e
        dp_scr[spot] = dp
        tile_top[spot] = top
        was = top_s[i]
        now = jnp.maximum(was, top)
        keep = jnp.exp2((was - now) * steep)
        take = jnp.exp2((top - now) * steep)
        top_s[i] = now
        sum_s[i] = sum_s[i] * keep + tile_sum * take
        del_s[i] = del_s[i] * keep + tile_del * take

    def grads(u, spot):
        old = unit_block[u]
        t = unit_tile[u]
        total = 1.0 / sum_s[old]
        weight = jnp.exp2((tile_top[spot] - top_s[old]) * steep) * total
        delta = del_s[old] * total
        p = e_scr[spot] * weight
        pb = p.astype(jnp.bfloat16)
        ds = (p * (dp_scr[spot] - delta)).astype(jnp.bfloat16)
        ot[old] += dot(values(t).T, pb, NN)
        dqt[old] += dot(keys(t).T, ds, NN)
        at = pl.ds(t, tile_blocks)
        dv[at] += dot(pb, rows_of(old, 1), NN).reshape(tile_blocks, BLK, HEAD)
        dk[at] += dot(ds, rows_of(old, 0), NN).reshape(tile_blocks, BLK, HEAD)

    def first(u, carry):
        scores(u, u)
        return carry

    def both(u, carry):
        spot = lax.rem(u, RING)
        grads(u - LAG, spot)
        scores(u, spot)
        return carry

    def last(n, carry):
        u = units + n
        grads(u - LAG, lax.rem(u, RING))
        return carry

    def several(n, carry):
        u = LAG + odd + MANY * n
        for m in range(MANY):
            grads(u + m - LAG, lax.rem(u + m, RING))
        for m in range(MANY):
            scores(u + m, lax.rem(u + m, RING))
        return carry

    odd = lax.rem(units - LAG, MANY)
    lax.fori_loop(0, LAG, first, 0, unroll=LAG)
    lax.fori_loop(LAG, LAG + odd, both, 0)
    lax.fori_loop(0, (units - LAG) // MANY, several, 0)
    lax.fori_loop(0, LAG, last, 0, unroll=LAG)

    def gone(t, carry):
        at = pl.ds(t * tile_blocks, tile_blocks)
        past = pl.ds(PAD + t * tile_blocks, tile_blocks)
        dkv[at, 0] = (dk[past] * scale).astype(jnp.bfloat16)
        dkv[at, 1] = dv[past].astype(jnp.bfloat16)
        return carry

    lax.fori_loop(0, tiles, gone, 0, unroll=2)
    for k in range(ys):
        for w in range(zs):
            part = dkv_out[k * zs + w]
            each_block(
                k, w, lambda b, x, j: pltpu.make_async_copy(dkv.at[b], part.at[x, :, j], dkv_sem).start()
            )

    def rows_out(i, carry):
        od[i // per, 0, i % per] = ot[i].T.astype(jnp.bfloat16).reshape(group, BLK, HEAD)
        od[i // per, 1, i % per] = (dqt[i].T * scale).astype(jnp.bfloat16).reshape(group, BLK, HEAD)
        pltpu.make_async_copy(od.at[i // per, :, i % per], od_out.at[i // per, :, i % per], od_sem).start()
        return carry

    lax.fori_loop(0, blocks, rows_out, 0, unroll=2)
    pltpu.make_async_copy(dkv, dkv, dkv_sem).wait()
    pltpu.make_async_copy(od, od, od_sem).wait()


def attention(assign, lengths, coord, qd, kv, *, xs, ys, zs):
    blocks = qd.shape[0] * qd.shape[2]
    group = qd.shape[3]
    slots = len(kv) * kv[0].shape[0] * kv[0].shape[2]
    rows = group * BLK
    f32, bf, i32 = jnp.float32, jnp.bfloat16, jnp.int32
    body = functools.partial(attend, docs=lengths.shape[0], slots=slots, group=group, xs=xs, ys=ys, zs=zs)
    smem = pl.BlockSpec(memory_space=pltpu.SMEM)
    far = pl.BlockSpec(memory_space=pltpu.HBM)
    return pl.pallas_call(
        body,
        out_shape=[jax.ShapeDtypeStruct(a.shape, bf) for a in (qd, *kv)],
        in_specs=[smem] * 3 + [far] * (1 + len(kv)),
        out_specs=[far] * (1 + len(kv)),
        scratch_shapes=[
            pltpu.VMEM(qd.shape, bf), pltpu.VMEM((PAD + slots, 2, BLK, HEAD), bf),
            pltpu.VMEM(qd.shape, bf), pltpu.VMEM((slots, 2, BLK, HEAD), bf),
            pltpu.VMEM((PAD + slots, BLK, HEAD), f32), pltpu.VMEM((PAD + slots, BLK, HEAD), f32),
            pltpu.VMEM((blocks, HEAD, rows), f32), pltpu.VMEM((blocks, HEAD, rows), f32),
            pltpu.VMEM((RING, TILE, rows), f32), pltpu.VMEM((RING, TILE, rows), f32),
            pltpu.VMEM((RING, 1, rows), f32),
            pltpu.VMEM((blocks, 1, rows), f32), pltpu.VMEM((blocks, 1, rows), f32),
            pltpu.VMEM((blocks, 1, rows), f32), pltpu.VMEM((blocks, 1, rows), i32),
            pltpu.VMEM((blocks, 1, rows), i32),
            pltpu.SMEM((blocks * SPAN,), i32), pltpu.SMEM((blocks * SPAN,), i32),
            pltpu.SemaphoreType.DMA, pltpu.SemaphoreType.DMA, pltpu.SemaphoreType.DMA, pltpu.SemaphoreType.DMA,
        ],
        compiler_params=pltpu.CompilerParams(vmem_limit_bytes=63 << 20),
        cost_estimate=pl.CostEstimate(flops=10 ** 9, bytes_accessed=8 << 20, transcendentals=0),
        name="attend",
    )(assign, lengths, coord, qd, *kv)


def lay_out(a_ref, b_ref, o_ref, *, xs, per, heads, copies):
    for which, ref in enumerate((a_ref, b_ref)):
        for x in range(xs):
            for h in range(heads):
                c = (x * heads + h) * HEAD
                block = ref[:, c:c + HEAD].reshape(per, BLK, HEAD)
                for n in range(copies):
                    if heads == 1:
                        o_ref[x * copies + n, which] = block
                    else:
                        o_ref[x * copies + n, which, :, h] = block


def spread(a, b, xs, copies):
    per = a.shape[0] // BLK
    heads = a.shape[1] // (xs * HEAD)
    shape = (xs * copies, 2, per) + ((heads,) if heads > 1 else ()) + (BLK, HEAD)
    return pl.pallas_call(
        functools.partial(lay_out, xs=xs, per=per, heads=heads, copies=copies),
        out_shape=jax.ShapeDtypeStruct(shape, a.dtype),
        cost_estimate=pl.CostEstimate(flops=10 ** 6, bytes_accessed=4 * a.size, transcendentals=0),
        name="spread",
    )(a, b)


def line_up(a_ref, p_ref, q_ref, *, xs, per, heads, copies):
    for which, ref in enumerate((p_ref, q_ref)):
        for x in range(xs):
            for h in range(heads):
                c = (x * heads + h) * HEAD
                if heads == 1:
                    block = a_ref[x * copies, which].astype(jnp.float32)
                    for n in range(1, copies):
                        block += a_ref[x * copies + n, which].astype(jnp.float32)
                    block = block.astype(jnp.bfloat16)
                else:
                    block = a_ref[x, which, :, h]
                ref[:, c:c + HEAD] = block.reshape(per * BLK, HEAD)


def gather(a, xs):
    copies, per = a.shape[0] // xs, a.shape[2]
    heads = a.shape[3] if a.ndim == 6 else 1
    out = jax.ShapeDtypeStruct((per * BLK, xs * heads * HEAD), a.dtype)
    return pl.pallas_call(
        functools.partial(line_up, xs=xs, per=per, heads=heads, copies=copies),
        out_shape=(out, out),
        cost_estimate=pl.CostEstimate(flops=10 ** 6, bytes_accessed=2 * a.size, transcendentals=0),
        compiler_params=pltpu.CompilerParams(vmem_limit_bytes=16 << 20),
        name="gather",
    )(a)


X, Y, Z = "ctx_0", "ctx_1", "ctx_2"
DP_CTX = ("dp", X, Y, Z)


def shift(k, size):
    return [(i, (i + k) % size) for i in range(size)]


def work(doc_lengths, assignment, queries, key_state_rows, value_state_rows, out_grad):
    xs, ys, zs = (lax.axis_size(name) for name in (X, Y, Z))
    coord = lax.axis_index((Y, Z)).reshape(1).astype(jnp.int32)

    kv = spread(key_state_rows, value_state_rows, xs, 1)
    kv = lax.all_to_all(kv, X, 0, 0, tiled=True)
    qd = spread(queries, out_grad, xs, 1)
    kv = [kv] + [lax.ppermute(kv, Z, shift(w, zs)) for w in range(1, zs)]
    parts = [kv]
    for k in range(1, ys):
        own = lax.ppermute(kv[0], Y, shift(k, ys))
        parts.append([own] + [lax.ppermute(part, Y, shift(k, ys)) for part in kv[1:]])
    kv = [part for row in parts for part in row]
    qd = lax.all_to_all(qd, X, 0, 0, tiled=True)

    od, *dkv = attention(assignment, doc_lengths, coord, qd, kv, xs=xs, ys=ys, zs=zs)

    def over_y(w):
        terms = [dkv[w]]
        for k in range(1, ys):
            terms.append(lax.ppermute(dkv[k * zs + w], Y, shift(k, ys)))
        return sum(part.astype(jnp.float32) for part in terms)

    other = [lax.ppermute(over_y(w).astype(jnp.bfloat16), Z, shift(w, zs)) for w in range(1, zs)]
    od = lax.all_to_all(od, X, 0, 0, tiled=True)
    dkv = sum([part.astype(jnp.float32) for part in other], over_y(0)).astype(jnp.bfloat16)
    dkv, od = lax.optimization_barrier((dkv, od))
    dkv = lax.all_to_all(dkv, X, 0, 0, tiled=True)
    return (*gather(od, xs), *gather(dkv, xs))


def solution(mesh):
    finer = Mesh(mesh.devices.reshape(mesh.shape["dp"], 4, 4, 2), DP_CTX)
    rows = P(DP_CTX, None)
    return jax.shard_map(
        work,
        mesh=finer,
        in_specs=(P("dp"), P("dp"), rows, rows, rows, rows),
        out_specs=(rows, rows, rows, rows),
        check_vma=False,
    )
```
